32 devices in a mesh: groups: 1, section: 2 (over x), axial: 16 (over z, y, core).
Axes of the slice: x: 2, y: 2, z: 4, core: 2. Of those that a mesh axis runs over, the one named last changes fastest.
Arguments:
- pair_in: bfloat16 [4, 128, 128, 128], P('groups', 'axial'), may hold values from -6 to 6
- crop_mask: int32 [4, 128], P('groups'), may hold values 0 or 1
- proj_weights: bfloat16 [2, 5, 128, 128], P('section'), may hold values from -0.5 to 0.5
- out_weights: bfloat16 [2, 128, 128], P('section'), may hold values from -0.5 to 0.5
- up_weights: bfloat16 [2, 128, 512], P('section'), may hold values from -0.5 to 0.5
- down_weights: bfloat16 [2, 512, 128], P('section'), may hold values from -0.25 to 0.25
- norm_gains: bfloat16 [2, 3, 128], P('section'), may hold values from 0.099609375 to 1.8984375
Outputs:
- pair_out: bfloat16 [4, 128, 128, 128], P(('groups', 'section'), 'axial')
The draws below stay inside these ranges and needn't reach their ends.
Inputs may be any that keep to these rules, and one draw needn't show every extreme that they name: `crop_mask`: 1 marks a residue inside the crop, 0 a padded one.
All inputs are finite; a program needn't handle non-finite values.
Results may differ from the reference program's by a relative error of at most 0.013.
Values may be sent and summed in bfloat16 or wider, within the bound.
A program may use at most 64 MiB of HBM per device.

```python
import jax
import jax.numpy as jnp
from jax import lax

C = 128
MB = 4
N = 128
BLOCKS = 2
FF = 512


def touch_ends(entries, key, smallest, high):
    extent = entries.shape
    place = [jax.random.randint(jax.random.fold_in(key, axis), (), 0, extent[axis]) for axis in range(len(extent))]
    entries = entries.at[tuple(place)].set(smallest)
    longest = extent.index(max(extent))
    place[longest] = (place[longest] + 1) % extent[longest]
    return entries.at[tuple(place)].set(high)


def shard_levels(key, extent, shards, smallest, largest):
    loudness = 1.0
    for axis_at, blocks in shards:
        steps = jax.random.uniform(jax.random.fold_in(jax.random.fold_in(key, 6), axis_at), (blocks,), jnp.float32, smallest / len(shards), largest / len(shards))
        loudness = loudness * jnp.repeat(jnp.exp(steps), extent[axis_at] // blocks).reshape((-1,) + (1,) * (len(extent) - 1 - axis_at))
    return loudness


def scatter_about(stream_key, dims, scale, reach, split=(), dtype=jnp.bfloat16):
    level = shard_levels(stream_key, dims, split, -0.22, 0.18) if split else 1.0
    drawn = jax.random.normal(stream_key, dims, jnp.float32) * scale * level
    return jnp.minimum(jnp.maximum(drawn, -reach), reach).astype(dtype)


def setup_inputs(seed: int = 0, part: int = 0) -> dict:
    splits = jax.random.split(jax.random.key(seed), 8)
    part_splits = jax.random.split(jax.random.fold_in(splits[7], part), 8)
    pair_in = scatter_about(part_splits[0], (MB, N, N, C), 1.0, 6.0, ((1, 16),))
    crop_mask = touch_ends((jax.random.randint(part_splits[1], (MB, N), 0, 8) < 7).astype(jnp.int32), jax.random.fold_in(part_splits[1], 1), 0, 1)
    proj_weights = scatter_about(splits[2], (BLOCKS, 5, C, C), C ** -0.5, 0.5, ((0, 2),))
    out_weights = scatter_about(splits[3], (BLOCKS, C, C), C ** -0.5, 0.5, ((0, 2),))
    up_weights = scatter_about(splits[4], (BLOCKS, C, FF), C ** -0.5, 0.5, ((0, 2),))
    down_weights = scatter_about(splits[5], (BLOCKS, FF, C), FF ** -0.5, 0.25, ((0, 2),))
    norm_gains = jnp.clip(1.0 + 0.18 * jax.random.normal(splits[6], (BLOCKS, 3, C), jnp.float32), 0.099609375, 1.8984375).astype(jnp.bfloat16)
    return dict(pair_in=pair_in, crop_mask=crop_mask, proj_weights=proj_weights, out_weights=out_weights, up_weights=up_weights, down_weights=down_weights, norm_gains=norm_gains)


epsilon = 1e-05

def normalize(values, axis_dim):
    center = values - lax.optimization_barrier(jnp.mean(values, axis=axis_dim, keepdims=True))
    spread = lax.optimization_barrier(jnp.mean(center * center, axis=axis_dim, keepdims=True))
    return center * lax.rsqrt(spread + epsilon)

def evo_block(current, mask_all, proj_mats, out_mat, up_mat, down_mat, gain_rows):
    channels = current.shape[2]
    gain_vals = gain_rows.astype(jnp.float32)
    pair_f = current.astype(jnp.float32)
    normed = (normalize(pair_f, 2) * gain_vals[0]).astype(jnp.bfloat16)
    linear = jnp.einsum('ijd,edc->ecij', normed.astype(jnp.float32), proj_mats[:4].astype(jnp.float32))
    pair_mask = mask_all[:, None] * mask_all[None, :]
    left_edge = (jax.nn.sigmoid(linear[1]) * linear[0] * pair_mask).astype(jnp.bfloat16)
    right_edge = (jax.nn.sigmoid(linear[3]) * linear[2] * pair_mask).astype(jnp.bfloat16)
    product = jnp.einsum('cik,cjk->cij', left_edge.astype(jnp.float32), right_edge.astype(jnp.float32)).astype(jnp.bfloat16)
    tri_norm = (normalize(product.astype(jnp.float32), 0) * gain_vals[1][:, None, None]).astype(jnp.bfloat16)
    update = jnp.einsum('cij,cd->ijd', tri_norm.astype(jnp.float32), out_mat.astype(jnp.float32))
    gate_values = jax.nn.sigmoid(jnp.einsum('ijd,dc->ijc', normed.astype(jnp.float32), proj_mats[4].astype(jnp.float32)))
    pair_mid = pair_f + gate_values * update
    trans_in = (normalize(pair_mid, 2) * gain_vals[2]).astype(jnp.bfloat16).reshape(-1, channels)
    hidden = jax.nn.relu(jnp.dot(trans_in, up_mat, preferred_element_type=jnp.float32)).astype(jnp.bfloat16)
    pair_new = pair_mid + jnp.dot(hidden, down_mat, preferred_element_type=jnp.float32).reshape(pair_mid.shape)
    return pair_new.astype(jnp.bfloat16)

def reference(pair_in, crop_mask, proj_weights, out_weights, up_weights, down_weights, norm_gains):
    finished = []
    for micro_index in range(MB):
        current = pair_in[micro_index]
        mask_all = crop_mask[micro_index].astype(jnp.float32)
        for layer_index in range(BLOCKS):
            current = evo_block(current, mask_all, proj_weights[layer_index], out_weights[layer_index], up_weights[layer_index], down_weights[layer_index], norm_gains[layer_index])
        finished.append(current)
    return jnp.stack(finished)
```

```python
import functools

import jax
import jax.numpy as jnp
from jax import lax
from jax.experimental import pallas as pl
from jax.experimental.pallas import tpu as pltpu
from jax.sharding import PartitionSpec as P

epsilon = 1e-05


def normalize(values, axis_dim):
    center = values - jnp.mean(values, axis=axis_dim, keepdims=True)
    spread = jnp.mean(center * center, axis=axis_dim, keepdims=True)
    return center * lax.rsqrt(spread + epsilon)


def triangle(pieces):
    return jnp.einsum(
        "gcik,gcjk->gcij", pieces[0], pieces[1], preferred_element_type=jnp.float32
    ).astype(jnp.bfloat16)


def evo_block(current, mask_all, proj_mats, out_mat, up_mat, down_mat, gain_rows):
    row_count = current.shape[0]
    width = current.shape[1]
    channels = current.shape[2]
    group_count = lax.axis_size("axial")
    per_group = channels // group_count
    row_start = lax.axis_index("axial") * row_count
    mask_rows = lax.dynamic_slice_in_dim(mask_all, row_start, row_count)
    gain_vals = gain_rows.astype(jnp.float32)
    pair_f = current.astype(jnp.float32)
    normed = (normalize(pair_f, 2) * gain_vals[0]).astype(jnp.bfloat16)
    linear = jnp.einsum("rnd,edc->ecrn", normed, proj_mats[:4], preferred_element_type=jnp.float32)
    pair_mask = mask_rows[:, None] * mask_all[None, :]
    left_edge = (jax.nn.sigmoid(linear[1]) * linear[0] * pair_mask).astype(jnp.bfloat16)
    right_edge = (jax.nn.sigmoid(linear[3]) * linear[2] * pair_mask).astype(jnp.bfloat16)
    left_groups = left_edge.reshape(group_count, per_group, row_count, width)
    right_groups = right_edge.reshape(group_count, per_group, row_count, width)
    product = triangle(
        (
            lax.all_to_all(left_groups, "axial", split_axis=0, concat_axis=2, tiled=True),
            lax.all_to_all(right_groups, "axial", split_axis=0, concat_axis=2, tiled=True),
        )
    )
    restored = lax.all_to_all(product, "axial", split_axis=2, concat_axis=0, tiled=True).reshape(
        channels, row_count, width
    )
    tri_norm = (normalize(restored.astype(jnp.float32), 0) * gain_vals[1][:, None, None]).astype(
        jnp.bfloat16
    )
    update = jnp.einsum("crn,cd->rnd", tri_norm, out_mat, preferred_element_type=jnp.float32)
    gate_values = jax.nn.sigmoid(
        jnp.einsum("rnd,dc->rnc", normed, proj_mats[4], preferred_element_type=jnp.float32)
    )
    pair_mid = pair_f + gate_values * update
    trans_in = (normalize(pair_mid, 2) * gain_vals[2]).astype(jnp.bfloat16).reshape(-1, channels)
    hidden = jax.nn.relu(jnp.dot(trans_in, up_mat, preferred_element_type=jnp.float32)).astype(
        jnp.bfloat16
    )
    pair_new = pair_mid + jnp.dot(hidden, down_mat, preferred_element_type=jnp.float32).reshape(
        pair_mid.shape
    )
    return pair_new.astype(jnp.bfloat16)


MESH = pl.DeviceIdType.MESH


def sigmoid(values):
    return 0.5 * jnp.tanh(0.5 * values) + 0.5


def normalize_rows(values, gain):
    scale = 1.0 / values.shape[0]
    center = values - jnp.sum(values, axis=0, keepdims=True) * scale
    spread = jnp.sum(center * center, axis=0, keepdims=True) * scale
    return center * lax.rsqrt(spread + epsilon) * gain


def matmul(mat, values):
    return lax.dot_general(mat, values, (((1,), (0,)), ((), ())), preferred_element_type=jnp.float32)


def fused_kernel(
    sections,
    peers,
    own_count,
    sub_rows,
    pair_ref,
    mask_ref,
    mask_smem,
    proj_ref,
    out_ref,
    up_ref,
    down_ref,
    gain_ref,
    result_ref,
    pair_buf,
    z_buf,
    normed_buf,
    gate_buf,
    edge_send,
    edge_recv,
    tri_send,
    tri_recv,
    left_f,
    right_f,
    tri_f,
    proj_all,
    out_all,
    up_all,
    down_all,
    gain_all,
    proj_t,
    out_t,
    up_t,
    down_t,
    gain_t,
    pair_sem,
    edge_send_sem,
    edge_recv_sem,
    tri_send_sem,
    tri_recv_sem,
    weight_send_sem,
    weight_sem,
):
    section = lax.axis_index("section")
    me = lax.axis_index("axial")
    rows, width, channels = pair_buf.shape[1:]
    per_group = channels // peers
    lanes = sub_rows * width
    steps = rows // sub_rows

    pair_copies = []
    for m in range(own_count):
        copy = pltpu.make_async_copy(
            pair_ref.at[section * own_count + m], pair_buf.at[m], pair_sem.at[m]
        )
        copy.start()
        pair_copies.append(copy)

    barrier = pltpu.get_barrier_semaphore()
    for k in range(1, peers):
        pl.semaphore_signal(
            barrier, inc=1, device_id={"axial": lax.rem(me + k, peers)}, device_id_type=MESH
        )
    for k in range(1, sections):
        pl.semaphore_signal(
            barrier,
            inc=1,
            device_id={"section": lax.rem(section + k, sections)},
            device_id_type=MESH,
        )
    pl.semaphore_wait(barrier, peers - 1 + sections - 1)

    weights = (
        (gain_ref, gain_all),
        (proj_ref, proj_all),
        (out_ref, out_all),
        (up_ref, up_all),
        (down_ref, down_all),
    )
    weight_copies = []
    for a, (source, gathered) in enumerate(weights):
        for k in range(1, sections):
            copy = pltpu.make_async_remote_copy(
                src_ref=source.at[0],
                dst_ref=gathered.at[section],
                send_sem=weight_send_sem.at[a, k],
                recv_sem=weight_sem.at[a, section],
                device_id={"section": lax.rem(section + k, sections)},
                device_id_type=MESH,
            )
            copy.start()
            weight_copies.append(copy)
        pltpu.make_async_copy(source.at[0], gathered.at[section], weight_sem.at[a, section]).start()

    def wait_weight(a, layer):
        source, gathered = weights[a]
        pltpu.make_async_copy(source.at[0], gathered.at[layer], weight_sem.at[a, layer]).wait()

    def turned(values):
        return values.astype(jnp.float32).T.astype(jnp.bfloat16)

    def prepare_gains(layer):
        wait_weight(0, layer)
        for index in range(gain_t.shape[1]):
            row = gain_all[layer, index : index + 1, :].astype(jnp.float32)
            gain_t[layer, index] = jnp.broadcast_to(row, (width, channels)).T

    def prepare_proj(layer):
        wait_weight(1, layer)
        for e in range(proj_t.shape[1]):
            proj_t[layer, e] = turned(proj_all[layer, e])

    def prepare_rest(layer):
        for a in (2, 3, 4):
            wait_weight(a, layer)
        out_t[layer] = turned(out_all[layer])
        up_t[layer] = turned(up_all[layer])
        down_t[layer] = turned(down_all[layer])

    def wide_gain(layer, index):
        return jnp.concatenate([gain_t[layer, index]] * sub_rows, axis=1)

    def load_pair(m):
        pair_copies[m].wait()

        def step(q, carry):
            for s in range(sub_rows):
                r = q * sub_rows + s
                z_buf[m, q, :, s * width : (s + 1) * width] = pair_buf[m, r].astype(jnp.float32).T
            return carry

        lax.fori_loop(0, steps, step, 0)

    def phase_norm(layer, m):
        def step(q, carry):
            normed_buf[m, q] = normalize_rows(z_buf[m, q], wide_gain(layer, 0)).astype(jnp.bfloat16)
            return carry

        lax.fori_loop(0, steps, step, 0)

    def phase_edges(layer, m):
        row_mask = mask_ref[pl.ds(section * own_count + m, 1), :].astype(jnp.float32)

        def step(q, carry):
            values = normed_buf[m, q]
            masks = []
            for s in range(sub_rows):
                own = mask_smem[section * own_count + m, me * rows + q * sub_rows + s]
                masks.append(row_mask * own.astype(jnp.float32))
            pair_mask = jnp.concatenate(masks, axis=1)
            for side in range(2):
                value = matmul(proj_t[layer, 2 * side], values)
                gate = matmul(proj_t[layer, 2 * side + 1], values)
                edge = sigmoid(gate) * value * pair_mask
                for s in range(sub_rows):
                    part = edge[:, s * width : (s + 1) * width].reshape(peers, per_group, width)
                    edge_send[m, :, side, q * sub_rows + s] = part.astype(jnp.bfloat16)
            return carry

        lax.fori_loop(0, steps, step, 0)

    def phase_gate(layer, m):
        def step(q, carry):
            gate_buf[m, q] = sigmoid(matmul(proj_t[layer, 4], normed_buf[m, q]))
            return carry

        lax.fori_loop(0, steps, step, 0)

    def edge_copy(m, peer):
        return pltpu.make_async_remote_copy(
            src_ref=edge_send.at[m, peer],
            dst_ref=edge_recv.at[m, me],
            send_sem=edge_send_sem.at[m, peer],
            recv_sem=edge_recv_sem.at[m, me],
            device_id={"axial": peer},
            device_id_type=MESH,
        )

    def tri_copy(m, peer):
        return pltpu.make_async_remote_copy(
            src_ref=tri_send.at[m, peer],
            dst_ref=tri_recv.at[m, me],
            send_sem=tri_send_sem.at[m, peer],
            recv_sem=tri_recv_sem.at[m, me],
            device_id={"axial": peer},
            device_id_type=MESH,
        )

    def send_all(make_copy, send, recv, recv_sem, m):
        pltpu.make_async_copy(send.at[m, me], recv.at[m, me], recv_sem.at[m, me]).start()

        def step(k, carry):
            make_copy(m, lax.rem(me + k, peers)).start()
            return carry

        lax.fori_loop(1, peers, step, 0)

    def wait_sent(make_copy, m):
        def step(k, carry):
            make_copy(m, lax.rem(me + k, peers)).wait_send()
            return carry

        lax.fori_loop(1, peers, step, 0)

    def wait_all(send, recv, recv_sem, m):
        def step(g, carry):
            pltpu.make_async_copy(send.at[m, g], recv.at[m, g], recv_sem.at[m, g]).wait()
            return carry

        lax.fori_loop(0, peers, step, 0)

    def phase_triangle(m):
        for g in range(peers):
            left_f[g * rows : (g + 1) * rows] = edge_recv[m, g, 0].astype(jnp.float32)
            right_f[g * rows : (g + 1) * rows] = edge_recv[m, g, 1].astype(jnp.float32)
        for c in range(per_group):
            tri_f[:, c, :] = lax.dot_general(
                left_f[:, c, :].astype(jnp.bfloat16),
                right_f[:, c, :].astype(jnp.bfloat16),
                (((1,), (1,)), ((), ())),
                preferred_element_type=jnp.float32,
            )
        for g in range(peers):
            tri_send[m, g] = tri_f[g * rows : (g + 1) * rows].astype(jnp.bfloat16)

    def phase_update(layer, m, last):
        def step(q, carry):
            parts = []
            for s in range(sub_rows):
                part = tri_recv[m, :, q * sub_rows + s].astype(jnp.float32)
                parts.append(part.reshape(channels, width))
            tri = jnp.concatenate(parts, axis=1)
            tri_norm = normalize_rows(tri, wide_gain(layer, 1)).astype(jnp.bfloat16)
            mid = z_buf[m, q] + gate_buf[m, q] * matmul(out_t[layer], tri_norm)
            trans_in = normalize_rows(mid, wide_gain(layer, 2)).astype(jnp.bfloat16)
            hidden = jnp.maximum(matmul(up_t[layer], trans_in), 0.0).astype(jnp.bfloat16)
            fresh = mid + matmul(down_t[layer], hidden)
            if last:
                for s in range(sub_rows):
                    part = fresh[:, s * width : (s + 1) * width]
                    result_ref[m, q * sub_rows + s] = part.T.astype(jnp.bfloat16)
            else:
                z_buf[m, q] = fresh.astype(jnp.bfloat16).astype(jnp.float32)
            return carry

        lax.fori_loop(0, steps, step, 0)

    edges = (edge_copy, edge_send, edge_recv, edge_recv_sem)
    tris = (tri_copy, tri_send, tri_recv, tri_recv_sem)
    everyone = range(own_count)
    for m in everyone:
        load_pair(m)
    prepare_gains(0)
    for m in everyone:
        phase_norm(0, m)
    prepare_proj(0)
    for m in everyone:
        phase_edges(0, m)
        send_all(*edges, m)
    for m in everyone:
        phase_gate(0, m)
    prepare_rest(0)
    for layer in range(1, sections):
        prepare_gains(layer)
        prepare_proj(layer)
        prepare_rest(layer)
    for layer in range(sections):
        last = layer == sections - 1
        for m in everyone:
            wait_all(*edges[1:], m)
            if layer > 0:
                wait_sent(tri_copy, m)
            phase_triangle(m)
            send_all(*tris, m)
        for m in everyone:
            wait_all(*tris[1:], m)
            phase_update(layer, m, last)
            wait_sent(edge_copy, m)
            if not last:
                phase_norm(layer + 1, m)
                phase_edges(layer + 1, m)
                send_all(*edges, m)
        if not last:
            for m in everyone:
                phase_gate(layer + 1, m)
    for m in everyone:
        wait_sent(tri_copy, m)
    for copy in weight_copies:
        copy.wait_send()


def fused_device(pair_in, crop_mask, proj_weights, out_weights, up_weights, down_weights, norm_gains):
    sections = lax.axis_size("section")
    peers = lax.axis_size("axial")
    micro_count, rows, width, channels = pair_in.shape
    own_count = micro_count // sections
    per_group = channels // peers
    sub_rows = 2 if rows % 2 == 0 else 1
    steps = rows // sub_rows
    lanes = sub_rows * width
    hidden = up_weights.shape[2]
    gains = norm_gains.shape[1]
    edge_kinds = proj_weights.shape[1]
    bf16, f32 = jnp.bfloat16, jnp.float32
    vmem = pl.BlockSpec(memory_space=pltpu.VMEM)
    dma = pltpu.SemaphoreType.DMA
    edge_shape = (own_count, peers, 2, rows, per_group, width)
    tri_shape = (own_count, peers, rows, per_group, width)
    wide_shape = (own_count, steps, channels, lanes)
    channel_shape = (peers * rows, per_group, width)
    return pl.pallas_call(
        functools.partial(fused_kernel, sections, peers, own_count, sub_rows),
        out_shape=jax.ShapeDtypeStruct((own_count, rows, width, channels), bf16),
        in_specs=[pl.BlockSpec(memory_space=pl.ANY), vmem, pl.BlockSpec(memory_space=pltpu.SMEM)]
        + [vmem] * 5,
        out_specs=vmem,
        scratch_shapes=[
            pltpu.VMEM((own_count, rows, width, channels), bf16),
            pltpu.VMEM(wide_shape, f32),
            pltpu.VMEM(wide_shape, bf16),
            pltpu.VMEM(wide_shape, f32),
            pltpu.VMEM(edge_shape, bf16),
            pltpu.VMEM(edge_shape, bf16),
            pltpu.VMEM(tri_shape, bf16),
            pltpu.VMEM(tri_shape, bf16),
            pltpu.VMEM(channel_shape, f32),
            pltpu.VMEM(channel_shape, f32),
            pltpu.VMEM(channel_shape, f32),
            pltpu.VMEM((sections,) + proj_weights.shape[1:], bf16),
            pltpu.VMEM((sections,) + out_weights.shape[1:], bf16),
            pltpu.VMEM((sections,) + up_weights.shape[1:], bf16),
            pltpu.VMEM((sections,) + down_weights.shape[1:], bf16),
            pltpu.VMEM((sections,) + norm_gains.shape[1:], bf16),
            pltpu.VMEM((sections, edge_kinds, channels, channels), bf16),
            pltpu.VMEM((sections, channels, channels), bf16),
            pltpu.VMEM((sections, hidden, channels), bf16),
            pltpu.VMEM((sections, channels, hidden), bf16),
            pltpu.VMEM((sections, gains, channels, width), f32),
            dma((own_count,)),
            dma((own_count, peers)),
            dma((own_count, peers)),
            dma((own_count, peers)),
            dma((own_count, peers)),
            dma((5, sections)),
            dma((5, sections)),
        ],
        compiler_params=pltpu.CompilerParams(
            collective_id=0, has_side_effects=True, vmem_limit_bytes=48 * 1024 * 1024
        ),
    )(
        pair_in,
        crop_mask,
        crop_mask,
        proj_weights,
        out_weights,
        up_weights,
        down_weights,
        norm_gains,
    )


def fits_fused(pair_in):
    channels, peers = pair_in.shape[3], lax.axis_size("axial")
    whole_tiles = channels % (8 * peers) == 0 and pair_in.shape[1] % 8 == 0
    return whole_tiles and pair_in.shape[2] % channels == 0


def per_device(pair_in, crop_mask, proj_weights, out_weights, up_weights, down_weights, norm_gains):
    if fits_fused(pair_in):
        return fused_device(
            pair_in, crop_mask, proj_weights, out_weights, up_weights, down_weights, norm_gains
        )
    section_index = lax.axis_index("section")
    section_count = lax.axis_size("section")
    micro_count = pair_in.shape[0]
    own_count = micro_count // section_count
    gathered = (
        lax.all_gather(proj_weights, "section", axis=0, tiled=True),
        lax.all_gather(out_weights, "section", axis=0, tiled=True),
        lax.all_gather(up_weights, "section", axis=0, tiled=True),
        lax.all_gather(down_weights, "section", axis=0, tiled=True),
        lax.all_gather(norm_gains, "section", axis=0, tiled=True),
    )
    own_pairs = lax.dynamic_slice_in_dim(pair_in, section_index * own_count, own_count, 0)
    own_masks = lax.dynamic_slice_in_dim(crop_mask, section_index * own_count, own_count, 0).astype(
        jnp.float32
    )
    outputs = []
    for member in range(own_count):
        current = own_pairs[member]
        for layer_index in range(section_count):
            current = evo_block(
                current,
                own_masks[member],
                gathered[0][layer_index],
                gathered[1][layer_index],
                gathered[2][layer_index],
                gathered[3][layer_index],
                gathered[4][layer_index],
            )
        outputs.append(current)
    return jnp.stack(outputs)


def solution(mesh):
    return jax.shard_map(
        per_device,
        mesh=mesh,
        in_specs=(
            P("groups", "axial", None, None),
            P("groups", None),
            P("section", None, None, None),
            P("section", None, None),
            P("section", None, None),
            P("section", None, None),
            P("section", None, None),
        ),
        out_specs=P(("groups", "section"), "axial", None, None),
        check_vma=False,
    )
```

```python
import functools

import jax
import jax.numpy as jnp
from jax import lax
from jax.experimental import pallas as pl
from jax.experimental.pallas import tpu as pltpu
from jax.sharding import PartitionSpec as P

epsilon = 1e-05


def normalize(values, axis_dim):
    center = values - jnp.mean(values, axis=axis_dim, keepdims=True)
    spread = jnp.mean(center * center, axis=axis_dim, keepdims=True)
    return center * lax.rsqrt(spread + epsilon)


def triangle(pieces):
    return jnp.einsum(
        "gcik,gcjk->gcij", pieces[0], pieces[1], preferred_element_type=jnp.float32
    ).astype(jnp.bfloat16)


def evo_block(current, mask_all, proj_mats, out_mat, up_mat, down_mat, gain_rows):
    row_count = current.shape[0]
    width = current.shape[1]
    channels = current.shape[2]
    group_count = lax.axis_size("axial")
    per_group = channels // group_count
    row_start = lax.axis_index("axial") * row_count
    mask_rows = lax.dynamic_slice_in_dim(mask_all, row_start, row_count)
    gain_vals = gain_rows.astype(jnp.float32)
    pair_f = current.astype(jnp.float32)
    normed = (normalize(pair_f, 2) * gain_vals[0]).astype(jnp.bfloat16)
    linear = jnp.einsum("rnd,edc->ecrn", normed, proj_mats[:4], preferred_element_type=jnp.float32)
    pair_mask = mask_rows[:, None] * mask_all[None, :]
    left_edge = (jax.nn.sigmoid(linear[1]) * linear[0] * pair_mask).astype(jnp.bfloat16)
    right_edge = (jax.nn.sigmoid(linear[3]) * linear[2] * pair_mask).astype(jnp.bfloat16)
    left_groups = left_edge.reshape(group_count, per_group, row_count, width)
    right_groups = right_edge.reshape(group_count, per_group, row_count, width)
    product = triangle(
        (
            lax.all_to_all(left_groups, "axial", split_axis=0, concat_axis=2, tiled=True),
            lax.all_to_all(right_groups, "axial", split_axis=0, concat_axis=2, tiled=True),
        )
    )
    restored = lax.all_to_all(product, "axial", split_axis=2, concat_axis=0, tiled=True).reshape(
        channels, row_count, width
    )
    tri_norm = (normalize(restored.astype(jnp.float32), 0) * gain_vals[1][:, None, None]).astype(
        jnp.bfloat16
    )
    update = jnp.einsum("crn,cd->rnd", tri_norm, out_mat, preferred_element_type=jnp.float32)
    gate_values = jax.nn.sigmoid(
        jnp.einsum("rnd,dc->rnc", normed, proj_mats[4], preferred_element_type=jnp.float32)
    )
    pair_mid = pair_f + gate_values * update
    trans_in = (normalize(pair_mid, 2) * gain_vals[2]).astype(jnp.bfloat16).reshape(-1, channels)
    hidden = jax.nn.relu(jnp.dot(trans_in, up_mat, preferred_element_type=jnp.float32)).astype(
        jnp.bfloat16
    )
    pair_new = pair_mid + jnp.dot(hidden, down_mat, preferred_element_type=jnp.float32).reshape(
        pair_mid.shape
    )
    return pair_new.astype(jnp.bfloat16)


MESH = pl.DeviceIdType.MESH


def sigmoid(values):
    return 0.5 * jnp.tanh(0.5 * values) + 0.5


def normalize_rows(values, gain):
    scale = 1.0 / values.shape[0]
    center = values - jnp.sum(values, axis=0, keepdims=True) * scale
    spread = jnp.sum(center * center, axis=0, keepdims=True) * scale
    return center * lax.rsqrt(spread + epsilon) * gain


def matmul(mat, values):
    return lax.dot_general(mat, values, (((1,), (0,)), ((), ())), preferred_element_type=jnp.float32)


def fused_kernel(
    sections,
    peers,
    halves,
    own_count,
    sub_rows,
    pair_ref,
    mask_ref,
    mask_smem,
    proj_ref,
    out_ref,
    up_ref,
    down_ref,
    gain_ref,
    result_ref,
    pair_buf,
    z_buf,
    normed_buf,
    gate_buf,
    edge_send,
    left_recv,
    right_recv,
    tri_send,
    tri_recv,
    left_f,
    right_f,
    tri_f,
    proj_all,
    out_all,
    up_all,
    down_all,
    gain_all,
    proj_t,
    out_t,
    up_t,
    down_t,
    gain_t,
    pair_sem,
    left_send_sem,
    left_recv_sem,
    right_send_sem,
    right_recv_sem,
    tri_send_sem,
    tri_recv_sem,
    weight_send_sem,
    weight_sem,
):
    section = lax.axis_index("section")
    me = lax.axis_index("axial")
    rows, width, channels = pair_buf.shape[1:]
    owners = peers // halves
    per_group = channels // owners
    my_half = me // owners
    my_owner = lax.rem(me, owners)
    steps = rows // sub_rows

    pair_copies = []
    for m in range(own_count):
        copy = pltpu.make_async_copy(
            pair_ref.at[section * own_count + m], pair_buf.at[m], pair_sem.at[m]
        )
        copy.start()
        pair_copies.append(copy)

    barrier = pltpu.get_barrier_semaphore()
    for k in range(1, peers):
        pl.semaphore_signal(
            barrier, inc=1, device_id={"axial": lax.rem(me + k, peers)}, device_id_type=MESH
        )
    for k in range(1, sections):
        pl.semaphore_signal(
            barrier,
            inc=1,
            device_id={"section": lax.rem(section + k, sections)},
            device_id_type=MESH,
        )
    pl.semaphore_wait(barrier, peers - 1 + sections - 1)

    weights = (
        (gain_ref, gain_all),
        (proj_ref, proj_all),
        (out_ref, out_all),
        (up_ref, up_all),
        (down_ref, down_all),
    )
    weight_copies = []
    for a, (source, gathered) in enumerate(weights):
        for k in range(1, sections):
            copy = pltpu.make_async_remote_copy(
                src_ref=source.at[0],
                dst_ref=gathered.at[section],
                send_sem=weight_send_sem.at[a, k],
                recv_sem=weight_sem.at[a, section],
                device_id={"section": lax.rem(section + k, sections)},
                device_id_type=MESH,
            )
            copy.start()
            weight_copies.append(copy)
        pltpu.make_async_copy(source.at[0], gathered.at[section], weight_sem.at[a, section]).start()

    def wait_weight(a, layer):
        source, gathered = weights[a]
        pltpu.make_async_copy(source.at[0], gathered.at[layer], weight_sem.at[a, layer]).wait()

    def turned(values):
        return values.astype(jnp.float32).T.astype(jnp.bfloat16)

    def prepare_gains(layer):
        wait_weight(0, layer)
        for index in range(gain_t.shape[1]):
            row = gain_all[layer, index : index + 1, :].astype(jnp.float32)
            gain_t[layer, index] = jnp.broadcast_to(row, (width, channels)).T

    def prepare_proj(layer):
        wait_weight(1, layer)
        for e in range(proj_t.shape[1]):
            proj_t[layer, e] = turned(proj_all[layer, e])

    def prepare_rest(layer):
        for a in (2, 3, 4):
            wait_weight(a, layer)
        out_t[layer] = turned(out_all[layer])
        up_t[layer] = turned(up_all[layer])
        down_t[layer] = turned(down_all[layer])

    def wide_gain(layer, index):
        return jnp.concatenate([gain_t[layer, index]] * sub_rows, axis=1)

    def load_pair(m):
        pair_copies[m].wait()

        def step(q, carry):
            for s in range(sub_rows):
                r = q * sub_rows + s
                z_buf[m, q, :, s * width : (s + 1) * width] = pair_buf[m, r].astype(jnp.float32).T
            return carry

        lax.fori_loop(0, steps, step, 0)

    def phase_norm(layer, m):
        def step(q, carry):
            normed_buf[m, q] = normalize_rows(z_buf[m, q], wide_gain(layer, 0)).astype(jnp.bfloat16)
            return carry

        lax.fori_loop(0, steps, step, 0)

    def phase_edges(layer, m):
        row_mask = mask_ref[pl.ds(section * own_count + m, 1), :].astype(jnp.float32)

        def step(q, carry):
            values = normed_buf[m, q]
            masks = []
            for s in range(sub_rows):
                own = mask_smem[section * own_count + m, me * rows + q * sub_rows + s]
                masks.append(row_mask * own.astype(jnp.float32))
            pair_mask = jnp.concatenate(masks, axis=1)
            for side in range(2):
                value = matmul(proj_t[layer, 2 * side], values)
                gate = matmul(proj_t[layer, 2 * side + 1], values)
                edge = sigmoid(gate) * value * pair_mask
                for s in range(sub_rows):
                    part = edge[:, s * width : (s + 1) * width].reshape(owners, per_group, width)
                    edge_send[m, :, side, q * sub_rows + s] = part.astype(jnp.bfloat16)
            return carry

        lax.fori_loop(0, steps, step, 0)

    def phase_gate(layer, m):
        def step(q, carry):
            gate_buf[m, q] = sigmoid(matmul(proj_t[layer, 4], normed_buf[m, q]))
            return carry

        lax.fori_loop(0, steps, step, 0)

    def left_copy(m, k):
        owner = lax.rem(my_owner + k, owners)
        return pltpu.make_async_remote_copy(
            src_ref=edge_send.at[m, owner, 0],
            dst_ref=left_recv.at[m, my_owner],
            send_sem=left_send_sem.at[m, k],
            recv_sem=left_recv_sem.at[m, my_owner],
            device_id={"axial": my_half * owners + owner},
            device_id_type=MESH,
        )

    def right_copy(slot, m, k):
        half = lax.rem(my_half + k // owners, halves)
        owner = lax.rem(my_owner + k % owners, owners)
        return pltpu.make_async_remote_copy(
            src_ref=edge_send.at[m, owner, 1],
            dst_ref=right_recv.at[slot, m, me],
            send_sem=right_send_sem.at[m, k],
            recv_sem=right_recv_sem.at[slot, m, me],
            device_id={"axial": half * owners + owner},
            device_id_type=MESH,
        )

    def tri_copy(m, k):
        owner = lax.rem(my_owner + k, owners)
        return pltpu.make_async_remote_copy(
            src_ref=tri_send.at[m, owner],
            dst_ref=tri_recv.at[m, my_owner],
            send_sem=tri_send_sem.at[m, k],
            recv_sem=tri_recv_sem.at[m, my_owner],
            device_id={"axial": my_half * owners + owner},
            device_id_type=MESH,
        )

    def send_edges(slot, m):
        pltpu.make_async_copy(
            edge_send.at[m, my_owner, 0],
            left_recv.at[m, my_owner],
            left_recv_sem.at[m, my_owner],
        ).start()
        pltpu.make_async_copy(
            edge_send.at[m, my_owner, 1],
            right_recv.at[slot, m, me],
            right_recv_sem.at[slot, m, me],
        ).start()
        for k in range(peers - 1, 0, -1):
            right_copy(slot, m, k).start()
        for k in range(owners - 1, 0, -1):
            left_copy(m, k).start()

    def wait_edges_sent(slot, m):
        for k in range(1, peers):
            right_copy(slot, m, k).wait_send()
        for k in range(1, owners):
            left_copy(m, k).wait_send()

    def send_tri(m):
        pltpu.make_async_copy(
            tri_send.at[m, my_owner], tri_recv.at[m, my_owner], tri_recv_sem.at[m, my_owner]
        ).start()
        for k in range(owners - 1, 0, -1):
            tri_copy(m, k).start()

    def wait_tri_sent(m):
        for k in range(1, owners):
            tri_copy(m, k).wait_send()

    def wait_left(m, g):
        pltpu.make_async_copy(left_recv.at[m, g], left_recv.at[m, g], left_recv_sem.at[m, g]).wait()

    def wait_right(slot, m, g):
        pltpu.make_async_copy(
            right_recv.at[slot, m, g], right_recv.at[slot, m, g], right_recv_sem.at[slot, m, g]
        ).wait()

    def wait_tri(m):
        for g in range(owners):
            pltpu.make_async_copy(tri_recv.at[m, g], tri_recv.at[m, g], tri_recv_sem.at[m, g]).wait()

    def phase_triangle(slot, m):
        for g in range(owners):
            wait_left(m, g)
            left_f[g * rows : (g + 1) * rows] = left_recv[m, g].astype(jnp.float32)
        for g in range(peers):
            wait_right(slot, m, g)
            right_f[g * rows : (g + 1) * rows] = right_recv[slot, m, g].astype(jnp.float32)
        for c in range(per_group):
            tri_f[:, c, :] = lax.dot_general(
                left_f[:, c, :].astype(jnp.bfloat16),
                right_f[:, c, :].astype(jnp.bfloat16),
                (((1,), (1,)), ((), ())),
                preferred_element_type=jnp.float32,
            )
        for g in range(owners):
            tri_send[m, g] = tri_f[g * rows : (g + 1) * rows].astype(jnp.bfloat16)

    def phase_update(layer, m, last):
        def step(q, carry):
            parts = []
            for s in range(sub_rows):
                part = tri_recv[m, :, q * sub_rows + s].astype(jnp.float32)
                parts.append(part.reshape(channels, width))
            tri = jnp.concatenate(parts, axis=1)
            tri_norm = normalize_rows(tri, wide_gain(layer, 1)).astype(jnp.bfloat16)
            mid = z_buf[m, q] + gate_buf[m, q] * matmul(out_t[layer], tri_norm)
            trans_in = normalize_rows(mid, wide_gain(layer, 2)).astype(jnp.bfloat16)
            hidden = jnp.maximum(matmul(up_t[layer], trans_in), 0.0).astype(jnp.bfloat16)
            fresh = mid + matmul(down_t[layer], hidden)
            if last:
                for s in range(sub_rows):
                    part = fresh[:, s * width : (s + 1) * width]
                    result_ref[m, q * sub_rows + s] = part.T.astype(jnp.bfloat16)
            else:
                z_buf[m, q] = fresh.astype(jnp.bfloat16).astype(jnp.float32)
            return carry

        lax.fori_loop(0, steps, step, 0)

    everyone = range(own_count)
    for m in everyone:
        load_pair(m)
    prepare_gains(0)
    for m in everyone:
        phase_norm(0, m)
    prepare_proj(0)
    for m in everyone:
        phase_edges(0, m)
        send_edges(0, m)
    for m in everyone:
        phase_gate(0, m)
    prepare_rest(0)
    for layer in range(1, sections):
        prepare_gains(layer)
        prepare_proj(layer)
        prepare_rest(layer)
    for layer in range(sections):
        last = layer == sections - 1
        for m in everyone:
            if layer > 0:
                wait_tri_sent(m)
            phase_triangle(layer % 2, m)
            send_tri(m)
        for m in everyone:
            wait_tri(m)
            phase_update(layer, m, last)
            wait_edges_sent(layer % 2, m)
            if not last:
                phase_norm(layer + 1, m)
                phase_edges(layer + 1, m)
                send_edges((layer + 1) % 2, m)
        if not last:
            for m in everyone:
                phase_gate(layer + 1, m)
    for m in everyone:
        wait_tri_sent(m)
    for copy in weight_copies:
        copy.wait_send()


def fused_device(pair_in, crop_mask, proj_weights, out_weights, up_weights, down_weights, norm_gains):
    sections = lax.axis_size("section")
    peers = lax.axis_size("axial")
    micro_count, rows, width, channels = pair_in.shape
    own_count = micro_count // sections
    halves = half_count(pair_in)
    owners = peers // halves
    per_group = channels // owners
    sub_rows = 2 if rows % 2 == 0 else 1
    steps = rows // sub_rows
    lanes = sub_rows * width
    hidden = up_weights.shape[2]
    gains = norm_gains.shape[1]
    edge_kinds = proj_weights.shape[1]
    bf16, f32 = jnp.bfloat16, jnp.float32
    vmem = pl.BlockSpec(memory_space=pltpu.VMEM)
    hbm = pl.BlockSpec(memory_space=pltpu.HBM)
    dma = pltpu.SemaphoreType.DMA
    edge_shape = (own_count, owners, 2, rows, per_group, width)
    left_shape = (own_count, owners, rows, per_group, width)
    right_shape = (2, own_count, peers, rows, per_group, width)
    wide_shape = (own_count, steps, channels, lanes)
    return pl.pallas_call(
        functools.partial(fused_kernel, sections, peers, halves, own_count, sub_rows),
        out_shape=jax.ShapeDtypeStruct((own_count, rows, width, channels), bf16),
        in_specs=[hbm, vmem, pl.BlockSpec(memory_space=pltpu.SMEM)] + [hbm] * 5,
        out_specs=vmem,
        scratch_shapes=[
            pltpu.VMEM((own_count, rows, width, channels), bf16),
            pltpu.VMEM(wide_shape, f32),
            pltpu.VMEM(wide_shape, bf16),
            pltpu.VMEM(wide_shape, f32),
            pltpu.VMEM(edge_shape, bf16),
            pltpu.VMEM(left_shape, bf16),
            pltpu.VMEM(right_shape, bf16),
            pltpu.VMEM(left_shape, bf16),
            pltpu.VMEM(left_shape, bf16),
            pltpu.VMEM((owners * rows, per_group, width), f32),
            pltpu.VMEM((peers * rows, per_group, width), f32),
            pltpu.VMEM((owners * rows, per_group, width), f32),
            pltpu.VMEM((sections,) + proj_weights.shape[1:], bf16),
            pltpu.VMEM((sections,) + out_weights.shape[1:], bf16),
            pltpu.VMEM((sections,) + up_weights.shape[1:], bf16),
            pltpu.VMEM((sections,) + down_weights.shape[1:], bf16),
            pltpu.VMEM((sections,) + norm_gains.shape[1:], bf16),
            pltpu.VMEM((sections, edge_kinds, channels, channels), bf16),
            pltpu.VMEM((sections, channels, channels), bf16),
            pltpu.VMEM((sections, hidden, channels), bf16),
            pltpu.VMEM((sections, channels, hidden), bf16),
            pltpu.VMEM((sections, gains, channels, width), f32),
            dma((own_count,)),
            dma((own_count, owners)),
            dma((own_count, owners)),
            dma((own_count, peers)),
            dma((2, own_count, peers)),
            dma((own_count, owners)),
            dma((own_count, owners)),
            dma((5, sections)),
            dma((5, sections)),
        ],
        compiler_params=pltpu.CompilerParams(
            collective_id=0, has_side_effects=True, vmem_limit_bytes=67043328
        ),
    )(
        pair_in,
        crop_mask,
        crop_mask,
        proj_weights,
        out_weights,
        up_weights,
        down_weights,
        norm_gains,
    )


def half_count(pair_in):
    peers = lax.axis_size("axial")
    return 2 if peers % 2 == 0 and pair_in.shape[3] % (8 * (peers // 2)) == 0 else 1


def fits_fused(pair_in):
    rows, width, channels = pair_in.shape[1:]
    owners = lax.axis_size("axial") // half_count(pair_in)
    return channels % (8 * owners) == 0 and rows % 8 == 0 and width % 128 == 0


def per_device(pair_in, crop_mask, proj_weights, out_weights, up_weights, down_weights, norm_gains):
    if fits_fused(pair_in):
        return fused_device(
            pair_in, crop_mask, proj_weights, out_weights, up_weights, down_weights, norm_gains
        )
    section_index = lax.axis_index("section")
    section_count = lax.axis_size("section")
    micro_count = pair_in.shape[0]
    own_count = micro_count // section_count
    gathered = (
        lax.all_gather(proj_weights, "section", axis=0, tiled=True),
        lax.all_gather(out_weights, "section", axis=0, tiled=True),
        lax.all_gather(up_weights, "section", axis=0, tiled=True),
        lax.all_gather(down_weights, "section", axis=0, tiled=True),
        lax.all_gather(norm_gains, "section", axis=0, tiled=True),
    )
    own_pairs = lax.dynamic_slice_in_dim(pair_in, section_index * own_count, own_count, 0)
    own_masks = lax.dynamic_slice_in_dim(crop_mask, section_index * own_count, own_count, 0).astype(
        jnp.float32
    )
    outputs = []
    for member in range(own_count):
        current = own_pairs[member]
        for layer_index in range(section_count):
            current = evo_block(
                current,
                own_masks[member],
                gathered[0][layer_index],
                gathered[1][layer_index],
                gathered[2][layer_index],
                gathered[3][layer_index],
                gathered[4][layer_index],
            )
        outputs.append(current)
    return jnp.stack(outputs)


def solution(mesh):
    return jax.shard_map(
        per_device,
        mesh=mesh,
        in_specs=(
            P("groups", "axial", None, None),
            P("groups", None),
            P("section", None, None, None),
            P("section", None, None),
            P("section", None, None),
            P("section", None, None),
            P("section", None, None),
        ),
        out_specs=P(("groups", "section"), "axial", None, None),
        check_vma=False,
    )
```

```python
import functools

import jax
import jax.numpy as jnp
from jax import lax
from jax.experimental import pallas as pl
from jax.experimental.pallas import tpu as pltpu
from jax.sharding import PartitionSpec as P

epsilon = 1e-05


def normalize(values, axis_dim):
    center = values - jnp.mean(values, axis=axis_dim, keepdims=True)
    spread = jnp.mean(center * center, axis=axis_dim, keepdims=True)
    return center * lax.rsqrt(spread + epsilon)


def triangle(pieces):
    return jnp.einsum(
        "gcik,gcjk->gcij", pieces[0], pieces[1], preferred_element_type=jnp.float32
    ).astype(jnp.bfloat16)


def evo_block(current, mask_all, proj_mats, out_mat, up_mat, down_mat, gain_rows):
    row_count = current.shape[0]
    width = current.shape[1]
    channels = current.shape[2]
    group_count = lax.axis_size("axial")
    per_group = channels // group_count
    row_start = lax.axis_index("axial") * row_count
    mask_rows = lax.dynamic_slice_in_dim(mask_all, row_start, row_count)
    gain_vals = gain_rows.astype(jnp.float32)
    pair_f = current.astype(jnp.float32)
    normed = (normalize(pair_f, 2) * gain_vals[0]).astype(jnp.bfloat16)
    linear = jnp.einsum("rnd,edc->ecrn", normed, proj_mats[:4], preferred_element_type=jnp.float32)
    pair_mask = mask_rows[:, None] * mask_all[None, :]
    left_edge = (jax.nn.sigmoid(linear[1]) * linear[0] * pair_mask).astype(jnp.bfloat16)
    right_edge = (jax.nn.sigmoid(linear[3]) * linear[2] * pair_mask).astype(jnp.bfloat16)
    left_groups = left_edge.reshape(group_count, per_group, row_count, width)
    right_groups = right_edge.reshape(group_count, per_group, row_count, width)
    product = triangle(
        (
            lax.all_to_all(left_groups, "axial", split_axis=0, concat_axis=2, tiled=True),
            lax.all_to_all(right_groups, "axial", split_axis=0, concat_axis=2, tiled=True),
        )
    )
    restored = lax.all_to_all(product, "axial", split_axis=2, concat_axis=0, tiled=True).reshape(
        channels, row_count, width
    )
    tri_norm = (normalize(restored.astype(jnp.float32), 0) * gain_vals[1][:, None, None]).astype(
        jnp.bfloat16
    )
    update = jnp.einsum("crn,cd->rnd", tri_norm, out_mat, preferred_element_type=jnp.float32)
    gate_values = jax.nn.sigmoid(
        jnp.einsum("rnd,dc->rnc", normed, proj_mats[4], preferred_element_type=jnp.float32)
    )
    pair_mid = pair_f + gate_values * update
    trans_in = (normalize(pair_mid, 2) * gain_vals[2]).astype(jnp.bfloat16).reshape(-1, channels)
    hidden = jax.nn.relu(jnp.dot(trans_in, up_mat, preferred_element_type=jnp.float32)).astype(
        jnp.bfloat16
    )
    pair_new = pair_mid + jnp.dot(hidden, down_mat, preferred_element_type=jnp.float32).reshape(
        pair_mid.shape
    )
    return pair_new.astype(jnp.bfloat16)


MESH = pl.DeviceIdType.MESH


def sigmoid(values):
    return 0.5 * jnp.tanh(0.5 * values) + 0.5


def normalize_rows(values, gain):
    scale = 1.0 / values.shape[0]
    center = values - jnp.sum(values, axis=0, keepdims=True) * scale
    spread = jnp.sum(center * center, axis=0, keepdims=True) * scale
    return center * lax.rsqrt(spread + epsilon) * gain


def matmul(mat, values):
    return lax.dot_general(mat, values, (((1,), (0,)), ((), ())), preferred_element_type=jnp.float32)


def fused_kernel(
    sections,
    peers,
    halves,
    own_count,
    sub_rows,
    pair_ref,
    mask_ref,
    mask_smem,
    proj_ref,
    out_ref,
    up_ref,
    down_ref,
    gain_ref,
    result_ref,
    pair_buf,
    z_buf,
    normed_buf,
    gate_buf,
    edge_send,
    left_recv,
    right_recv,
    tri_send,
    tri_recv,
    left_f,
    right_f,
    tri_f,
    proj_all,
    out_all,
    up_all,
    down_all,
    gain_all,
    proj_t,
    out_t,
    up_t,
    down_t,
    gain_t,
    pair_sem,
    left_send_sem,
    left_recv_sem,
    right_send_sem,
    right_recv_sem,
    tri_send_sem,
    tri_recv_sem,
    weight_send_sem,
    weight_sem,
):
    section = lax.axis_index("section")
    me = lax.axis_index("axial")
    rows, width, channels = pair_buf.shape[1:]
    owners = peers // halves
    per_group = channels // owners
    my_half = me // owners
    my_owner = lax.rem(me, owners)
    steps = rows // sub_rows

    pair_copies = []
    for m in range(own_count):
        copy = pltpu.make_async_copy(
            pair_ref.at[section * own_count + m], pair_buf.at[m], pair_sem.at[m]
        )
        copy.start()
        pair_copies.append(copy)

    barrier = pltpu.get_barrier_semaphore()
    for k in range(1, peers):
        pl.semaphore_signal(
            barrier, inc=1, device_id={"axial": lax.rem(me + k, peers)}, device_id_type=MESH
        )
    for k in range(1, sections):
        pl.semaphore_signal(
            barrier,
            inc=1,
            device_id={"section": lax.rem(section + k, sections)},
            device_id_type=MESH,
        )
    weights = (
        (gain_ref, gain_all, None),
        (proj_ref, proj_all, (2, 2)),
        (proj_ref, proj_all, (0, 2)),
        (proj_ref, proj_all, (4, 1)),
        (out_ref, out_all, None),
        (up_ref, up_all, None),
        (down_ref, down_all, None),
    )

    def weight_part(ref, layer, span):
        return ref.at[layer] if span is None else ref.at[layer, pl.ds(*span)]

    for a, (source, gathered, span) in enumerate(weights):
        pltpu.make_async_copy(
            weight_part(source, 0, span),
            weight_part(gathered, section, span),
            weight_sem.at[a, section],
        ).start()

    def send_weights():
        copies = []
        for a, (_, gathered, span) in enumerate(weights):
            for k in range(1, sections):
                copy = pltpu.make_async_remote_copy(
                    src_ref=weight_part(gathered, section, span),
                    dst_ref=weight_part(gathered, section, span),
                    send_sem=weight_send_sem.at[a, k],
                    recv_sem=weight_sem.at[a, section],
                    device_id={"section": lax.rem(section + k, sections)},
                    device_id_type=MESH,
                )
                copy.start()
                copies.append(copy)
        return copies

    def wait_weight(a, layer):
        part = weight_part(weights[a][1], layer, weights[a][2])
        pltpu.make_async_copy(part, part, weight_sem.at[a, layer]).wait()

    def turned(values):
        return values.astype(jnp.float32).T.astype(jnp.bfloat16)

    def prepare_gains(layer):
        wait_weight(0, layer)
        for index in range(gain_t.shape[1]):
            row = gain_all[layer, index : index + 1, :].astype(jnp.float32)
            gain_t[layer, index] = jnp.broadcast_to(row, (width, channels)).T

    def prepare_proj(layer, side):
        wait_weight(2 - side, layer)
        for e in (2 * side, 2 * side + 1):
            proj_t[layer, e] = turned(proj_all[layer, e])

    def prepare_rest(layer):
        wait_weight(3, layer)
        proj_t[layer, 4] = turned(proj_all[layer, 4])
        for a in (4, 5, 6):
            wait_weight(a, layer)
        out_t[layer] = turned(out_all[layer])
        up_t[layer] = turned(up_all[layer])
        down_t[layer] = turned(down_all[layer])

    def prepare_all(layer):
        prepare_gains(layer)
        prepare_proj(layer, 1)
        prepare_proj(layer, 0)
        prepare_rest(layer)

    def wide_gain(layer, index):
        return jnp.concatenate([gain_t[layer, index]] * sub_rows, axis=1)

    def load_pair(m):
        pair_copies[m].wait()

        def step(q, carry):
            for s in range(sub_rows):
                r = q * sub_rows + s
                z_buf[m, q, :, s * width : (s + 1) * width] = pair_buf[m, r].astype(jnp.float32).T
            return carry

        lax.fori_loop(0, steps, step, 0, unroll=True)

    def phase_norm(layer, m):
        def step(q, carry):
            normed_buf[m, q] = normalize_rows(z_buf[m, q], wide_gain(layer, 0)).astype(jnp.bfloat16)
            return carry

        lax.fori_loop(0, steps, step, 0, unroll=True)

    def phase_edges(layer, m, side):
        row_mask = mask_ref[pl.ds(section * own_count + m, 1), :].astype(jnp.float32)

        def step(q, carry):
            values = normed_buf[m, q]
            masks = []
            for s in range(sub_rows):
                own = mask_smem[section * own_count + m, me * rows + q * sub_rows + s]
                masks.append(row_mask * own.astype(jnp.float32))
            pair_mask = jnp.concatenate(masks, axis=1)
            value = matmul(proj_t[layer, 2 * side], values)
            gate = matmul(proj_t[layer, 2 * side + 1], values)
            edge = sigmoid(gate) * value * pair_mask
            for s in range(sub_rows):
                part = edge[:, s * width : (s + 1) * width].reshape(owners, per_group, width)
                edge_send[m, :, side, q * sub_rows + s] = part.astype(jnp.bfloat16)
            return carry

        lax.fori_loop(0, steps, step, 0, unroll=True)

    def phase_gate(layer, m):
        def step(q, carry):
            gate_buf[m, q] = sigmoid(matmul(proj_t[layer, 4], normed_buf[m, q]))
            return carry

        lax.fori_loop(0, steps, step, 0, unroll=True)

    def left_copy(m, k):
        owner = lax.rem(my_owner + k, owners)
        return pltpu.make_async_remote_copy(
            src_ref=edge_send.at[m, owner, 0],
            dst_ref=left_recv.at[m, my_owner],
            send_sem=left_send_sem.at[m, k],
            recv_sem=left_recv_sem.at[m, my_owner],
            device_id={"axial": my_half * owners + owner},
            device_id_type=MESH,
        )

    def right_copy(slot, m, k):
        half = lax.rem(my_half + k // owners, halves)
        owner = lax.rem(my_owner + k % owners, owners)
        return pltpu.make_async_remote_copy(
            src_ref=edge_send.at[m, owner, 1],
            dst_ref=right_recv.at[slot, m, me],
            send_sem=right_send_sem.at[m, k],
            recv_sem=right_recv_sem.at[slot, m, me],
            device_id={"axial": half * owners + owner},
            device_id_type=MESH,
        )

    def tri_copy(m, k):
        owner = lax.rem(my_owner + k, owners)
        return pltpu.make_async_remote_copy(
            src_ref=tri_send.at[m, owner],
            dst_ref=tri_recv.at[m, my_owner],
            send_sem=tri_send_sem.at[m, k],
            recv_sem=tri_recv_sem.at[m, my_owner],
            device_id={"axial": my_half * owners + owner},
            device_id_type=MESH,
        )

    def send_right(slot, m):
        pltpu.make_async_copy(
            edge_send.at[m, my_owner, 1],
            right_recv.at[slot, m, me],
            right_recv_sem.at[slot, m, me],
        ).start()
        for k in range(peers - 1, 0, -1):
            right_copy(slot, m, k).start()

    def send_left(m):
        pltpu.make_async_copy(
            edge_send.at[m, my_owner, 0],
            left_recv.at[m, my_owner],
            left_recv_sem.at[m, my_owner],
        ).start()
        for k in range(owners - 1, 0, -1):
            left_copy(m, k).start()

    def wait_edges_sent(slot, m):
        for k in range(1, peers):
            right_copy(slot, m, k).wait_send()
        for k in range(1, owners):
            left_copy(m, k).wait_send()

    def send_tri(m):
        pltpu.make_async_copy(
            tri_send.at[m, my_owner], tri_recv.at[m, my_owner], tri_recv_sem.at[m, my_owner]
        ).start()
        for k in range(owners - 1, 0, -1):
            tri_copy(m, k).start()

    def wait_tri_sent(m):
        for k in range(1, owners):
            tri_copy(m, k).wait_send()

    def wait_left(m, g):
        pltpu.make_async_copy(left_recv.at[m, g], left_recv.at[m, g], left_recv_sem.at[m, g]).wait()

    def wait_right(slot, m, g):
        pltpu.make_async_copy(
            right_recv.at[slot, m, g], right_recv.at[slot, m, g], right_recv_sem.at[slot, m, g]
        ).wait()

    def wait_tri(m):
        for g in range(owners):
            pltpu.make_async_copy(tri_recv.at[m, g], tri_recv.at[m, g], tri_recv_sem.at[m, g]).wait()

    def phase_triangle(slot, m):
        for g in range(owners):
            wait_left(m, g)
            left_f[g * rows : (g + 1) * rows] = left_recv[m, g].astype(jnp.float32)
        for g in range(peers):
            wait_right(slot, m, g)
            right_f[g * rows : (g + 1) * rows] = right_recv[slot, m, g].astype(jnp.float32)
        for c in range(per_group):
            tri_f[:, c, :] = lax.dot_general(
                left_f[:, c, :].astype(jnp.bfloat16),
                right_f[:, c, :].astype(jnp.bfloat16),
                (((1,), (1,)), ((), ())),
                preferred_element_type=jnp.float32,
            )
        for g in range(owners):
            tri_send[m, g] = tri_f[g * rows : (g + 1) * rows].astype(jnp.bfloat16)

    def phase_update(layer, m, last):
        def step(q, carry):
            parts = []
            for s in range(sub_rows):
                part = tri_recv[m, :, q * sub_rows + s].astype(jnp.float32)
                parts.append(part.reshape(channels, width))
            tri = jnp.concatenate(parts, axis=1)
            tri_norm = normalize_rows(tri, wide_gain(layer, 1)).astype(jnp.bfloat16)
            mid = z_buf[m, q] + gate_buf[m, q] * matmul(out_t[layer], tri_norm)
            trans_in = normalize_rows(mid, wide_gain(layer, 2)).astype(jnp.bfloat16)
            hidden = jnp.maximum(matmul(up_t[layer], trans_in), 0.0).astype(jnp.bfloat16)
            fresh = mid + matmul(down_t[layer], hidden)
            if last:
                for s in range(sub_rows):
                    part = fresh[:, s * width : (s + 1) * width]
                    result_ref[m, q * sub_rows + s] = part.T.astype(jnp.bfloat16)
            else:
                z_buf[m, q] = fresh.astype(jnp.bfloat16).astype(jnp.float32)
            return carry

        lax.fori_loop(0, steps, step, 0, unroll=True)

    everyone = range(own_count)
    for m in everyone:
        load_pair(m)
    prepare_all(section)

    @pl.when(section == 0)
    def early_edges():
        for m in everyone:
            phase_norm(0, m)
            phase_edges(0, m, 1)
            phase_edges(0, m, 0)

    pl.semaphore_wait(barrier, peers - 1 + sections - 1)
    weight_copies = send_weights()

    @pl.when(section != 0)
    def late_norm():
        prepare_gains(0)
        for m in everyone:
            phase_norm(0, m)

    for m in everyone:
        for side in (1, 0):

            @pl.when(section != 0)
            def late_edges():
                if m == 0:
                    prepare_proj(0, side)
                phase_edges(0, m, side)

            if side:
                send_right(0, m)
            else:
                send_left(m)

    @pl.when(section != 0)
    def late_rest():
        prepare_rest(0)

    for m in everyone:
        phase_gate(0, m)

    for layer in range(1, sections):

        @pl.when(section != layer)
        def other_weights():
            prepare_all(layer)

    for layer in range(sections):
        last = layer == sections - 1
        for m in everyone:
            if layer > 0:
                wait_tri_sent(m)
            phase_triangle(layer % 2, m)
            send_tri(m)
        for m in everyone:
            wait_tri(m)
            phase_update(layer, m, last)
            wait_edges_sent(layer % 2, m)
            if not last:
                phase_norm(layer + 1, m)
                phase_edges(layer + 1, m, 1)
                send_right((layer + 1) % 2, m)
                phase_edges(layer + 1, m, 0)
                send_left(m)
        if not last:
            for m in everyone:
                phase_gate(layer + 1, m)
    for m in everyone:
        wait_tri_sent(m)
    for copy in weight_copies:
        copy.wait_send()


def fused_device(pair_in, crop_mask, proj_weights, out_weights, up_weights, down_weights, norm_gains):
    sections = lax.axis_size("section")
    peers = lax.axis_size("axial")
    micro_count, rows, width, channels = pair_in.shape
    own_count = micro_count // sections
    halves = half_count(pair_in)
    owners = peers // halves
    per_group = channels // owners
    sub_rows = 2 if rows % 2 == 0 else 1
    steps = rows // sub_rows
    lanes = sub_rows * width
    hidden = up_weights.shape[2]
    gains = norm_gains.shape[1]
    edge_kinds = proj_weights.shape[1]
    bf16, f32 = jnp.bfloat16, jnp.float32
    vmem = pl.BlockSpec(memory_space=pltpu.VMEM)
    hbm = pl.BlockSpec(memory_space=pltpu.HBM)
    dma = pltpu.SemaphoreType.DMA
    edge_shape = (own_count, owners, 2, rows, per_group, width)
    left_shape = (own_count, owners, rows, per_group, width)
    right_shape = (2, own_count, peers, rows, per_group, width)
    wide_shape = (own_count, steps, channels, lanes)
    return pl.pallas_call(
        functools.partial(fused_kernel, sections, peers, halves, own_count, sub_rows),
        out_shape=jax.ShapeDtypeStruct((own_count, rows, width, channels), bf16),
        in_specs=[hbm, vmem, pl.BlockSpec(memory_space=pltpu.SMEM)] + [hbm] * 5,
        out_specs=vmem,
        scratch_shapes=[
            pltpu.VMEM((own_count, rows, width, channels), bf16),
            pltpu.VMEM(wide_shape, f32),
            pltpu.VMEM(wide_shape, bf16),
            pltpu.VMEM(wide_shape, f32),
            pltpu.VMEM(edge_shape, bf16),
            pltpu.VMEM(left_shape, bf16),
            pltpu.VMEM(right_shape, bf16),
            pltpu.VMEM(left_shape, bf16),
            pltpu.VMEM(left_shape, bf16),
            pltpu.VMEM((owners * rows, per_group, width), f32),
            pltpu.VMEM((peers * rows, per_group, width), f32),
            pltpu.VMEM((owners * rows, per_group, width), f32),
            pltpu.VMEM((sections,) + proj_weights.shape[1:], bf16),
            pltpu.VMEM((sections,) + out_weights.shape[1:], bf16),
            pltpu.VMEM((sections,) + up_weights.shape[1:], bf16),
            pltpu.VMEM((sections,) + down_weights.shape[1:], bf16),
            pltpu.VMEM((sections,) + norm_gains.shape[1:], bf16),
            pltpu.VMEM((sections, edge_kinds, channels, channels), bf16),
            pltpu.VMEM((sections, channels, channels), bf16),
            pltpu.VMEM((sections, hidden, channels), bf16),
            pltpu.VMEM((sections, channels, hidden), bf16),
            pltpu.VMEM((sections, gains, channels, width), f32),
            dma((own_count,)),
            dma((own_count, owners)),
            dma((own_count, owners)),
            dma((own_count, peers)),
            dma((2, own_count, peers)),
            dma((own_count, owners)),
            dma((own_count, owners)),
            dma((7, sections)),
            dma((7, sections)),
        ],
        compiler_params=pltpu.CompilerParams(
            collective_id=0, has_side_effects=True, vmem_limit_bytes=67043328
        ),
    )(
        pair_in,
        crop_mask,
        crop_mask,
        proj_weights,
        out_weights,
        up_weights,
        down_weights,
        norm_gains,
    )


def half_count(pair_in):
    peers = lax.axis_size("axial")
    return 2 if peers % 2 == 0 and pair_in.shape[3] % (8 * (peers // 2)) == 0 else 1


def fits_fused(pair_in):
    rows, width, channels = pair_in.shape[1:]
    owners = lax.axis_size("axial") // half_count(pair_in)
    return channels % (8 * owners) == 0 and rows % 8 == 0 and width % 128 == 0


def per_device(pair_in, crop_mask, proj_weights, out_weights, up_weights, down_weights, norm_gains):
    if fits_fused(pair_in):
        return fused_device(
            pair_in, crop_mask, proj_weights, out_weights, up_weights, down_weights, norm_gains
        )
    section_index = lax.axis_index("section")
    section_count = lax.axis_size("section")
    micro_count = pair_in.shape[0]
    own_count = micro_count // section_count
    gathered = (
        lax.all_gather(proj_weights, "section", axis=0, tiled=True),
        lax.all_gather(out_weights, "section", axis=0, tiled=True),
        lax.all_gather(up_weights, "section", axis=0, tiled=True),
        lax.all_gather(down_weights, "section", axis=0, tiled=True),
        lax.all_gather(norm_gains, "section", axis=0, tiled=True),
    )
    own_pairs = lax.dynamic_slice_in_dim(pair_in, section_index * own_count, own_count, 0)
    own_masks = lax.dynamic_slice_in_dim(crop_mask, section_index * own_count, own_count, 0).astype(
        jnp.float32
    )
    outputs = []
    for member in range(own_count):
        current = own_pairs[member]
        for layer_index in range(section_count):
            current = evo_block(
                current,
                own_masks[member],
                gathered[0][layer_index],
                gathered[1][layer_index],
                gathered[2][layer_index],
                gathered[3][layer_index],
                gathered[4][layer_index],
            )
        outputs.append(current)
    return jnp.stack(outputs)


def solution(mesh):
    return jax.shard_map(
        per_device,
        mesh=mesh,
        in_specs=(
            P("groups", "axial", None, None),
            P("groups", None),
            P("section", None, None, None),
            P("section", None, None),
            P("section", None, None),
            P("section", None, None),
            P("section", None, None),
        ),
        out_specs=P(("groups", "section"), "axial", None, None),
        check_vma=False,
    )
```
